32 devices in a mesh: span: 4 (over z), cols: 2 (over y), copy: 4 (over x, core).
Axes of the slice: x: 2, y: 2, z: 4, core: 2. Of those that a mesh axis runs over, the one named last changes fastest.
Arguments:
- leak_rate: float32 [8, 512, 2560], P('copy', 'span', 'cols'), parts along dimension 0, may hold values from 0.2 to 2
- signal_in: bfloat16 [8, 512, 2560], P('copy', 'span', 'cols'), parts along dimension 0, may hold values from -6 to 6
- gate_in: bfloat16 [8, 512, 2560], P('copy', 'span', 'cols'), parts along dimension 0, may hold values from -6 to 6
Outputs:
- sequence_out: bfloat16 [8, 512, 2560], P('copy', 'span', 'cols'), parts along dimension 0
The draws below stay inside these ranges and needn't reach their ends.
There are 4 independent parts, one for each index of `copy`. The reference program is written for one: setup_inputs(seed, part) draws one part's arguments, and reference() takes and returns one part's arrays. A program takes and returns all parts, laid end to end along the dimension named above; each array names one. Nothing has to cross between parts.
All inputs are finite; a program needn't handle non-finite values.
Results may differ from the reference program's by a relative error of at most 0.001.
Values sent between devices are 32-bit elements; how exact they have to be, the bound alone decides.
A program may use at most 64 MiB of HBM per device.

```python
import jax
import jax.numpy as jnp
from jax import lax

BATCH = 2
CHANNELS = 2560
LENGTH = 512


def shard_levels(rng, dims, cuts, least, high):
    level = 1.0
    for axis_at, shards_of in cuts:
        draws = jax.random.uniform(jax.random.fold_in(jax.random.fold_in(rng, 6), axis_at), (shards_of,), jnp.float32, least / len(cuts), high / len(cuts))
        level = level * jnp.repeat(jnp.exp(draws), dims[axis_at] // shards_of).reshape((-1,) + (1,) * (len(dims) - 1 - axis_at))
    return level


def noise(stream_key, shape, spread, reach, cuts=(), kind=jnp.bfloat16):
    factor_of = shard_levels(stream_key, shape, cuts, -0.22, 0.18) if cuts else 1.0
    result = jax.random.normal(stream_key, shape, jnp.float32) * spread * factor_of
    return jnp.minimum(jnp.maximum(result, -reach), reach).astype(kind)


def setup_inputs(seed: int = 0, part: int = 0) -> dict:
    arg_keys = jax.random.split(jax.random.key(seed), 4)
    part_splits = jax.random.split(jax.random.fold_in(arg_keys[3], part), 4)
    leak_rate = jnp.clip(0.2 + 1.8 * jax.random.uniform(part_splits[0], (BATCH, LENGTH, CHANNELS), jnp.float32) ** shard_levels(part_splits[0], (BATCH, LENGTH, CHANNELS), ((1, 4), (2, 2)), -0.2, 0.2), 0.2, 2.0)
    signal_in = noise(part_splits[1], (BATCH, LENGTH, CHANNELS), 1.0, 6.0, ((1, 4), (2, 2)))
    gate_in = noise(part_splits[2], (BATCH, LENGTH, CHANNELS), 1.0, 6.0, ((1, 4), (2, 2)))
    return dict(leak_rate=leak_rate, signal_in=signal_in, gate_in=gate_in)


def join_pair(earlier, later):
    return earlier[0] * later[0], later[0] * earlier[1] + later[1]


def reference(leak_rate, signal_in, gate_in):
    keep = jnp.exp(-leak_rate / LENGTH)
    push = signal_in.astype(jnp.float32) * LENGTH ** -0.5
    forward = lax.associative_scan(join_pair, (keep, push), axis=1)[1]
    backward = lax.associative_scan(join_pair, (keep, push), axis=1, reverse=True)[1]
    states = forward + backward
    gated = states * jax.nn.silu(gate_in.astype(jnp.float32))
    sequence_out = gated.astype(jnp.bfloat16)
    return sequence_out
```

```python
import functools
import math

import jax
import jax.numpy as jnp
from jax import lax
from jax.experimental import pallas as pl
from jax.experimental.pallas import tpu as pltpu
from jax.sharding import PartitionSpec as P

LANES = 128
SUBS = 8


def kernel(
    n, total, batch, length, groups, pitch, parts,
    leak_hbm, signal_hbm, gate_hbm, out_ref,
    leak_v, signal_v, gate_v, keep_s, push_s, silu_s, w_s, u_s, v_s, local_s,
    left_s, left_r, right_s, right_r, ahead_s, behind_s,
    in_sem, left_send, left_recv, right_send, right_recv, ready,
):
    me = lax.axis_index("span")
    steps = length // SUBS
    chunks = leak_v.shape[0]
    rows = batch * groups
    every = chunks * rows
    width = groups * LANES
    first_part = parts[0]
    head, tail = first_part * rows, (chunks - first_part) * rows
    MESH = pl.DeviceIdType.MESH

    def fetch(which, c):
        source = (leak_hbm, signal_hbm, gate_hbm)[which]
        target = (leak_v, signal_v, gate_v)[which]
        lanes = pl.ds(pl.multiple_of(c * width, width), width)
        return pltpu.make_async_copy(source.at[:, :, lanes], target.at[c], in_sem.at[which, c])

    for c in range(chunks):
        fetch(0, c).start()
        fetch(1, c).start()

    barrier = pltpu.get_barrier_semaphore()

    def greet(p, carry):
        pl.semaphore_signal(barrier, inc=1, device_id={"span": p}, device_id_type=MESH)
        return carry

    lax.fori_loop(me + 1, n, greet, 0)

    def left(source, p, start, size, k):
        return pltpu.make_async_remote_copy(
            src_ref=left_s.at[pl.ds(start, size)],
            dst_ref=left_r.at[source, pl.ds(start, size)],
            send_sem=left_send.at[p, k],
            recv_sem=left_recv.at[source, k],
            device_id={"span": p},
            device_id_type=MESH,
        )

    def right(source, p, size):
        return pltpu.make_async_remote_copy(
            src_ref=right_s.at[pl.ds(0, size)],
            dst_ref=right_r.at[source, pl.ds(0, size)],
            send_sem=right_send.at[p],
            recv_sem=right_recv.at[source],
            device_id={"span": p},
            device_id_type=MESH,
        )

    def each(begin, end, act):
        lax.fori_loop(begin, end, lambda p, x: (act(p), x)[1], 0)

    @pl.when(me > 0)
    def _():
        pl.semaphore_wait(barrier, me)

    def arrived(p):
        pl.semaphore_signal(ready.at[me], inc=1, device_id={"span": p}, device_id_type=MESH)

    each(0, me, arrived)

    def spread(target, c, row, value):
        for s in range(SUBS):
            target[c, row, pl.ds(s * pitch, steps), :] = value[s * steps:(s + 1) * steps]

    def at(ref, c, r, k):
        return ref[c, r, pl.ds(k, SUBS, stride=pitch), :]

    place = lax.broadcasted_iota(jnp.int32, (SUBS, LANES), 0)

    def from_before(x, d, fill):
        return jnp.where(place < d, fill, pltpu.roll(x, d, 0))

    def from_after(x, d, fill):
        return jnp.where(place >= SUBS - d, fill, pltpu.roll(x, SUBS - d, 0))

    rate = -math.log2(math.e) / total

    def leftward(c, carry):
        fetch(0, c).wait()
        fetch(1, c).wait()
        for b in range(batch):
            for g in range(groups):
                lanes = pl.ds(g * LANES, LANES)
                spread(keep_s, c, b * groups + g, jnp.exp2(leak_v[c, b, :, lanes] * rate))
                spread(push_s, c, b * groups + g, signal_v[c, b, :, lanes].astype(jnp.float32))
        for r in range(rows):
            q, g = at(keep_s, c, r, 0), at(push_s, c, r, 0)
            for k in range(1, steps):
                g = g + q * at(push_s, c, r, k)
                q = q * at(keep_s, c, r, k)
            local_s[c, 2, r] = q
            d = 1
            while d < SUBS:
                g = g + q * from_after(g, d, 0.0)
                q = q * from_after(q, d, 1.0)
                d *= 2
            local_s[c, 1, r] = g
            local_s[c, 3, r] = q
            row = c * rows + r
            left_s[pl.ds(row, 1), :] = g[:1]
            left_s[pl.ds(every + row, 1), :] = q[:1]
        return carry

    edge = me == n - 1

    lax.fori_loop(0, first_part, leftward, 0)

    @pl.when(edge)
    def _():
        left(me, 0, 0, head, 0).start()

    lax.fori_loop(first_part, chunks, leftward, 0)

    @pl.when(edge)
    def _():
        left(me, 0, head, tail, 1).start()
        each(1, me, lambda p: left(me, p, 0, every, 0).start())

    @pl.when(~edge)
    def _():
        each(0, me, lambda p: left(me, p, 0, 2 * every, 0).start())

    for c in range(chunks):
        fetch(2, c).start()

    def rightward(c, carry):
        for r in range(rows):
            f = at(push_s, c, r, 0)
            for k in range(1, steps):
                f = at(keep_s, c, r, k) * f + at(push_s, c, r, k)
            q = local_s[c, 2, r]
            d = 1
            while d < SUBS:
                f = f + q * from_before(f, d, 0.0)
                q = q * from_before(q, d, 1.0)
                d *= 2
            local_s[c, 0, r] = f
            local_s[c, 2, r] = q
            row = c * rows + r
            right_s[pl.ds(row, 1), :] = f[SUBS - 1:]
            right_s[pl.ds(every + row, 1), :] = q[SUBS - 1:]
        return carry

    lax.fori_loop(0, chunks, rightward, 0)

    scale = total ** (-0.5)

    def second(c, carry):
        fetch(2, c).wait()
        for b in range(batch):
            for g in range(groups):
                x = gate_v[c, b, :, pl.ds(g * LANES, LANES)].astype(jnp.float32)
                spread(silu_s, c, b * groups + g, (x * scale) / (1.0 + jnp.exp(-x)))
        for r in range(rows):
            f = from_before(local_s[c, 0, r], 1, 0.0)
            u = from_before(local_s[c, 2, r], 1, 1.0)
            for k in range(steps):
                keep = at(keep_s, c, r, k)
                f = keep * f + at(push_s, c, r, k)
                u = u * keep
                w_s[c, r, pl.ds(k, SUBS, stride=pitch), :] = f
                u_s[c, r, pl.ds(k, SUBS, stride=pitch), :] = u * at(silu_s, c, r, k)
            g = from_after(local_s[c, 1, r], 1, 0.0)
            v = from_after(local_s[c, 3, r], 1, 1.0)
            for k in reversed(range(steps)):
                keep, silu = at(keep_s, c, r, k), at(silu_s, c, r, k)
                g = keep * g + at(push_s, c, r, k)
                v = v * keep
                w_s[c, r, pl.ds(k, SUBS, stride=pitch), :] = (at(w_s, c, r, k) + g) * silu
                v_s[c, r, pl.ds(k, SUBS, stride=pitch), :] = v * silu
        return carry

    lax.fori_loop(0, chunks, second, 0)

    def onward(size):
        def act(p):
            pl.semaphore_wait(ready.at[p], 1)
            right(me, p, size).start()
        each(me + 1, n, act)

    @pl.when(me == 0)
    def _():
        onward(every)

    @pl.when(me > 0)
    def _():
        onward(2 * every)

    @pl.when(me > 0)
    def _():
        def join(i, state):
            s, q = state
            j = me - i
            right(j, me, 2 * every).wait_recv()
            return (
                s + q * right_r[j, pl.ds(0, every), :],
                q * right_r[j, pl.ds(every, every), :],
            )

        zero = jnp.zeros((every, LANES), jnp.float32)
        s, q = lax.fori_loop(1, me, join, (zero, zero + 1.0))
        right(0, me, every).wait_recv()
        ahead_s[...] = s + q * right_r[0, pl.ds(0, every), :]

        def entering(c, carry):
            for r in range(rows):
                ahead = ahead_s[pl.ds(c * rows + r, 1), :]
                for s in range(SUBS):
                    span = pl.ds(s * pitch, steps)
                    w_s[c, r, span, :] = w_s[c, r, span, :] + u_s[c, r, span, :] * ahead
            return carry

        lax.fori_loop(0, chunks, entering, 0)

    @pl.when(edge)
    def _():
        left(me, 0, 0, head, 0).wait_send()
        left(me, 0, head, tail, 1).wait_send()
        each(1, me, lambda p: left(me, p, 0, every, 0).wait_send())

    @pl.when(~edge)
    def _():
        each(0, me, lambda p: left(me, p, 0, 2 * every, 0).wait_send())

    @pl.when(me == 0)
    def _():
        each(1, n, lambda p: right(me, p, every).wait_send())

    @pl.when(me > 0)
    def _():
        each(me + 1, n, lambda p: right(me, p, 2 * every).wait_send())

    def leave(c, carry):
        for b in range(batch):
            for g in range(groups):
                r = b * groups + g
                behind = behind_s[pl.ds(c * rows + r, 1), :]
                lanes = pl.ds(pl.multiple_of(c * width + g * LANES, LANES), LANES)
                for s in range(SUBS):
                    span = pl.ds(s * pitch, steps)
                    out_ref[b, pl.ds(s * steps, steps), lanes] = (
                        w_s[c, r, span, :] + v_s[c, r, span, :] * behind
                    ).astype(out_ref.dtype)
        return carry

    def join(j, state):
        s, q = state
        left(j, me, 0, 2 * every, 0).wait_recv()
        return s + q * left_r[j, pl.ds(0, every), :], q * left_r[j, pl.ds(every, every), :]

    zero = jnp.zeros((every, LANES), jnp.float32)
    near, far = lax.fori_loop(me + 1, n - 1, join, (zero, zero + 1.0))

    def behind(begin, end):
        if end > begin:
            behind_s[begin:end] = near[begin:end] + far[begin:end] * left_r[n - 1, begin:end]

    @pl.when(edge)
    def _():
        behind_s[...] = zero

    @pl.when((me > 0) & ~edge)
    def _():
        left(n - 1, me, 0, every, 0).wait_recv()
        behind(0, every)

    @pl.when(me == 0)
    def _():
        left(n - 1, 0, 0, head, 0).wait_recv()
        behind(0, head)

    lax.fori_loop(0, first_part, leave, 0)

    @pl.when(me == 0)
    def _():
        left(n - 1, 0, head, tail, 1).wait_recv()
        behind(head, every)

    lax.fori_loop(first_part, chunks, leave, 0)


def body(leak_rate, signal_in, gate_in):
    n = lax.axis_size("span")
    batch, length, channels = leak_rate.shape
    total = length * n
    blocks = channels // LANES
    groups = next(g for g in (2, 5, 1) if blocks % g == 0)
    chunks = blocks // groups
    rows = batch * groups
    steps = length // SUBS
    pitch = steps + 4
    first_part = max(1, (3 * chunks) // 5)
    hbm = pl.BlockSpec(memory_space=pl.ANY)
    f32 = jnp.float32
    spread = pltpu.VMEM((chunks, rows, SUBS * pitch, LANES), f32)
    every = chunks * rows
    return pl.pallas_call(
        functools.partial(kernel, n, total, batch, length, groups, pitch, (first_part,)),
        out_shape=pltpu.VMEM(leak_rate.shape, jnp.bfloat16),
        in_specs=[hbm] * 3,
        out_specs=pl.BlockSpec(memory_space=pltpu.VMEM),
        scratch_shapes=[
            pltpu.VMEM((chunks, batch, length, groups * LANES), f32),
            pltpu.VMEM((chunks, batch, length, groups * LANES), jnp.bfloat16),
            pltpu.VMEM((chunks, batch, length, groups * LANES), jnp.bfloat16),
            spread, spread, spread, spread, spread, spread,
            pltpu.VMEM((chunks, 4, rows, SUBS, LANES), f32),
            pltpu.VMEM((2 * every, LANES), f32),
            pltpu.VMEM((n, 2 * every, LANES), f32),
            pltpu.VMEM((2 * every, LANES), f32),
            pltpu.VMEM((n, 2 * every, LANES), f32),
            pltpu.VMEM((every, LANES), f32),
            pltpu.VMEM((every, LANES), f32),
            pltpu.SemaphoreType.DMA((3, chunks)),
            pltpu.SemaphoreType.DMA((n, 2)),
            pltpu.SemaphoreType.DMA((n, 2)),
            pltpu.SemaphoreType.DMA((n,)),
            pltpu.SemaphoreType.DMA((n,)),
            pltpu.SemaphoreType.REGULAR((n,)),
        ],
        compiler_params=pltpu.CompilerParams(collective_id=0, has_side_effects=True),
    )(leak_rate, signal_in, gate_in)


def solution(mesh):
    spec = P("copy", "span", "cols")
    return jax.shard_map(body, mesh=mesh, in_specs=(spec,) * 3, out_specs=spec, check_vma=False)
```

```python
import functools
import math

import jax
import jax.numpy as jnp
from jax import lax
from jax.experimental import pallas as pl
from jax.experimental.pallas import tpu as pltpu
from jax.sharding import PartitionSpec as P

LANES = 128
SUBS = 8
MESH = pl.DeviceIdType.MESH


def kernel(
    n, total, batch, length, cuts, per, pitch,
    leak_hbm, signal_hbm, gate_hbm, out_ref,
    leak_v, signal_v, gate_v, keep_s, push_s, silu_s, w_s, u_s, v_s, local_s,
    left_s, left_r, right_s, right_r, ahead_s, behind_s,
    sems, recv, ready,
):
    me = lax.axis_index("span")
    first, edge = me == 0, me == n - 1
    steps = length // SUBS
    tiles = cuts[-1]
    units = tiles * batch
    head = cuts[1] * batch
    trips = tiles // per

    def fetch(which, i):
        source = (leak_hbm, signal_hbm)[which]
        target = (leak_v, signal_v)[which]
        lanes = pl.ds(cuts[i] * LANES, (cuts[i + 1] - cuts[i]) * LANES)
        return pltpu.make_async_copy(
            source.at[:, :, lanes], target.at[:, :, lanes], sems.at[2 * i + which]
        )

    for i in range(len(cuts) - 1):
        fetch(0, i).start()
        fetch(1, i).start()

    def each(begin, end, act):
        lax.fori_loop(begin, end, lambda p, x: (act(p), x)[1], 0)

    barrier = pltpu.get_barrier_semaphore()

    def greet(p):
        pl.semaphore_signal(barrier, inc=1, device_id={"span": p}, device_id_type=MESH)

    def arrived(p):
        pl.semaphore_signal(ready, inc=1, device_id={"span": p}, device_id_type=MESH)

    each(me + 1, n, greet)

    @pl.when(~first)
    def _():
        pl.semaphore_wait(barrier, me)

    each(0, me, arrived)

    def left(source, p, start, size, second=False):
        return pltpu.make_async_remote_copy(
            src_ref=left_s.at[pl.ds(start, size)],
            dst_ref=left_r.at[source, pl.ds(start, size)],
            send_sem=sems.at[source if second else p],
            recv_sem=recv.at[p if second else source],
            device_id={"span": p},
            device_id_type=MESH,
        )

    def right(source, p, size):
        return pltpu.make_async_remote_copy(
            src_ref=right_s.at[pl.ds(0, size)],
            dst_ref=right_r.at[source, pl.ds(0, size)],
            send_sem=sems.at[p],
            recv_sem=recv.at[source],
            device_id={"span": p},
            device_id_type=MESH,
        )

    def spread(target, u, value):
        for s in range(SUBS):
            target[u, pl.ds(s * pitch, steps), :] = value[s * steps:(s + 1) * steps]

    def at(ref, u, k):
        return ref[u, pl.ds(k, SUBS, stride=pitch), :]

    place = lax.broadcasted_iota(jnp.int32, (SUBS, LANES), 0)

    def from_before(x, d, fill):
        return jnp.where(place < d, fill, pltpu.roll(x, d, 0))

    def from_after(x, d, fill):
        return jnp.where(place >= SUBS - d, fill, pltpu.roll(x, SUBS - d, 0))

    rate = -math.log2(math.e) / total

    def leftward(u):
        b, lanes = u % batch, pl.ds(u // batch * LANES, LANES)
        spread(keep_s, u, jnp.exp2(leak_v[b, :, lanes] * rate))
        spread(push_s, u, signal_v[b, :, lanes].astype(jnp.float32))
        q, g = at(keep_s, u, 0), at(push_s, u, 0)
        for k in range(1, steps):
            g = g + q * at(push_s, u, k)
            q = q * at(keep_s, u, k)
        local_s[u, 1] = g
        local_s[u, 2] = q
        d = 1
        while d < SUBS:
            g = g + q * pltpu.roll(g, SUBS - d, 0)
            q = q * pltpu.roll(q, SUBS - d, 0)
            d *= 2
        left_s[u:u + 1] = g[:1]

    for i in range(len(cuts) - 1):
        fetch(0, i).wait()
        fetch(1, i).wait()
        for u in range(cuts[i] * batch, cuts[i + 1] * batch):
            leftward(u)
        if i == 0:
            @pl.when(edge)
            def _():
                left(me, 0, 0, head).start()

    @pl.when(edge)
    def _():
        left(me, 0, head, units - head, True).start()

    gates = pltpu.make_async_copy(gate_hbm, gate_v, sems.at[n])
    gates.start()

    def rightward(t, carry):
        for i in range(per * batch):
            u = t * (per * batch) + i
            f = at(push_s, u, 0)
            for k in range(1, steps):
                f = at(keep_s, u, k) * f + at(push_s, u, k)
            g, q = local_s[u, 1], local_s[u, 2]
            a = q
            d = 1
            while d < SUBS:
                f = f + q * from_before(f, d, 0.0)
                g = g + a * from_after(g, d, 0.0)
                q = q * from_before(q, d, 1.0)
                a = a * from_after(a, d, 1.0)
                d *= 2
            local_s[u, 0] = f
            local_s[u, 1] = g
            local_s[u, 2] = q
            local_s[u, 3] = a
            right_s[pl.ds(u, 1), :] = f[SUBS - 1:]
            right_s[pl.ds(units + u, 1), :] = q[SUBS - 1:]
            left_s[pl.ds(units + u, 1), :] = a[:1]
        return carry

    lax.fori_loop(0, trips, rightward, 0)

    @pl.when(edge)
    def _():
        each(1, me, lambda p: left(me, p, 0, units).start())

    @pl.when(~edge)
    def _():
        each(0, me, lambda p: left(me, p, 0, 2 * units).start())

    scale = total ** (-0.5)
    gates.wait()

    def second(t, carry):
        for i in range(per * batch):
            u = t * (per * batch) + i
            lanes = pl.ds(pl.multiple_of((t * per + i // batch) * LANES, LANES), LANES)
            x = gate_v[i % batch, :, lanes].astype(jnp.float32)
            spread(silu_s, u, (x * scale) / (1.0 + jnp.exp(-x)))
        for i in range(per * batch):
            u = t * (per * batch) + i
            f = from_before(local_s[u, 0], 1, 0.0)
            a = from_before(local_s[u, 2], 1, 1.0)
            for k in range(steps):
                keep = at(keep_s, u, k)
                f = keep * f + at(push_s, u, k)
                a = a * keep
                w_s[u, pl.ds(k, SUBS, stride=pitch), :] = f
                u_s[u, pl.ds(k, SUBS, stride=pitch), :] = a * at(silu_s, u, k)
            g = from_after(local_s[u, 1], 1, 0.0)
            a = from_after(local_s[u, 3], 1, 1.0)
            for k in reversed(range(steps)):
                keep, silu = at(keep_s, u, k), at(silu_s, u, k)
                g = keep * g + at(push_s, u, k)
                a = a * keep
                w_s[u, pl.ds(k, SUBS, stride=pitch), :] = (at(w_s, u, k) + g) * silu
                v_s[u, pl.ds(k, SUBS, stride=pitch), :] = a * silu
        return carry

    lax.fori_loop(0, trips, second, 0)

    @pl.when(~edge)
    def _():
        pl.semaphore_wait(ready, n - 1 - me)

    @pl.when(first)
    def _():
        each(1, n, lambda p: right(me, p, units).start())

    @pl.when(~first)
    def _():
        each(me + 1, n, lambda p: right(me, p, 2 * units).start())

    zero = jnp.zeros((units, LANES), jnp.float32)

    @pl.when(~first)
    def _():
        def join(i, state):
            s, q = state
            j = me - i
            right(j, me, 2 * units).wait_recv()
            return s + q * right_r[j, :units], q * right_r[j, units:]

        s, q = lax.fori_loop(1, me, join, (zero, zero + 1.0))
        right(0, me, units).wait_recv()
        ahead_s[...] = s + q * right_r[0, :units]

        def entering(t, carry):
            for i in range(per * batch):
                u = t * (per * batch) + i
                ahead = ahead_s[pl.ds(u, 1), :]
                for s in range(SUBS):
                    rows = pl.ds(s * pitch, steps)
                    w_s[u, rows, :] = w_s[u, rows, :] + u_s[u, rows, :] * ahead
            return carry

        lax.fori_loop(0, trips, entering, 0)

    @pl.when(edge)
    def _():
        left(me, 0, 0, head).wait_send()
        left(me, 0, head, units - head, True).wait_send()
        each(1, me, lambda p: left(me, p, 0, units).wait_send())

    @pl.when(~edge)
    def _():
        each(0, me, lambda p: left(me, p, 0, 2 * units).wait_send())

    @pl.when(first)
    def _():
        each(1, n, lambda p: right(me, p, units).wait_send())

    @pl.when(~first)
    def _():
        each(me + 1, n, lambda p: right(me, p, 2 * units).wait_send())

    def join(j, state):
        s, q = state
        left(j, me, 0, 2 * units).wait_recv()
        return s + q * left_r[j, :units], q * left_r[j, units:]

    near, far = lax.fori_loop(me + 1, n - 1, join, (zero, zero + 1.0))

    def behind(begin, end):
        behind_s[begin:end] = near[begin:end] + far[begin:end] * left_r[n - 1, begin:end]

    def leave(begin, end):
        for u in range(begin, end):
            b, lanes = u % batch, pl.ds(u // batch * LANES, LANES)
            state = behind_s[u:u + 1]
            for s in range(SUBS):
                rows = pl.ds(s * pitch, steps)
                out_ref[b, pl.ds(s * steps, steps), lanes] = (
                    w_s[u, rows, :] + v_s[u, rows, :] * state
                ).astype(out_ref.dtype)

    @pl.when(edge)
    def _():
        behind_s[...] = zero

    @pl.when(~first & ~edge)
    def _():
        left(n - 1, me, 0, units).wait_recv()
        behind(0, units)

    @pl.when(first)
    def _():
        left(n - 1, 0, 0, head).wait_recv()
        behind(0, head)

    leave(0, head)

    @pl.when(first)
    def _():
        left(n - 1, 0, head, units - head, True).wait_recv()
        behind(head, units)

    leave(head, units)


def body(leak_rate, signal_in, gate_in):
    n = lax.axis_size("span")
    batch, length, channels = leak_rate.shape
    tiles = channels // LANES
    cuts = sorted({0, -(-tiles * 3 // 5), tiles})
    per = 2 if tiles % 2 == 0 else 1
    units = tiles * batch
    pitch = length // SUBS + 4
    hbm = pl.BlockSpec(memory_space=pl.ANY)
    f32 = jnp.float32
    spread = pltpu.VMEM((units, SUBS * pitch, LANES), f32)
    dma, regular = pltpu.SemaphoreType.DMA, pltpu.SemaphoreType.REGULAR
    return pl.pallas_call(
        functools.partial(kernel, n, length * n, batch, length, cuts, per, pitch),
        out_shape=pltpu.VMEM(leak_rate.shape, jnp.bfloat16),
        in_specs=[hbm] * 3,
        out_specs=pl.BlockSpec(memory_space=pltpu.VMEM),
        scratch_shapes=[
            pltpu.VMEM(leak_rate.shape, f32),
            pltpu.VMEM(leak_rate.shape, signal_in.dtype),
            pltpu.VMEM(leak_rate.shape, gate_in.dtype),
            spread, spread, spread, spread, spread, spread,
            pltpu.VMEM((units, 4, SUBS, LANES), f32),
            pltpu.VMEM((2 * units, LANES), f32),
            pltpu.VMEM((n, 2 * units, LANES), f32),
            pltpu.VMEM((2 * units, LANES), f32),
            pltpu.VMEM((n, 2 * units, LANES), f32),
            pltpu.VMEM((units, LANES), f32),
            pltpu.VMEM((units, LANES), f32),
            dma((max(2 * len(cuts) - 2, n + 1),)), dma((n,)), regular,
        ],
        compiler_params=pltpu.CompilerParams(collective_id=0, has_side_effects=True),
    )(leak_rate, signal_in, gate_in)


def solution(mesh):
    spec = P("copy", "span", "cols")
    return jax.shard_map(body, mesh=mesh, in_specs=(spec,) * 3, out_specs=spec, check_vma=False)
```

```python
import functools
import math

import jax
import jax.numpy as jnp
from jax import lax
from jax.experimental import pallas as pl
from jax.experimental.pallas import tpu as pltpu
from jax.sharding import PartitionSpec as P

LANES = 128
SUBS = 8
MESH = pl.DeviceIdType.MESH


def kernel(
    n, total, batch, length, cuts, per, pitch,
    leak_hbm, signal_hbm, gate_hbm, out_ref,
    leak_v, signal_v, gate_v, keep_s, push_s, silu_s, w_s, u_s, v_s, local_s,
    left_s, left_r, right_s, right_r, ahead_s, behind_s,
    recv, ready,
):
    me = lax.axis_index("span")
    first, edge = me == 0, me == n - 1
    steps = length // SUBS
    tiles = cuts[-1]
    units = tiles * batch
    head = cuts[len(cuts) // 2] * batch
    trips = tiles // per

    def left(sems, source, p, start, size, second=False):
        return pltpu.make_async_remote_copy(
            src_ref=left_s.at[pl.ds(start, size)],
            dst_ref=left_r.at[source, pl.ds(start, size)],
            send_sem=sems.at[source if second else p],
            recv_sem=recv.at[p if second else source],
            device_id={"span": p},
            device_id_type=MESH,
        )

    def right(sems, source, p, size):
        return pltpu.make_async_remote_copy(
            src_ref=right_s.at[pl.ds(0, size)],
            dst_ref=right_r.at[source, pl.ds(0, size)],
            send_sem=sems.at[p],
            recv_sem=recv.at[source],
            device_id={"span": p},
            device_id_type=MESH,
        )

    zero = jnp.zeros((units, LANES), jnp.float32)

    def begin(sems):
        def fetch(which, i):
            source = (leak_hbm, signal_hbm)[which]
            target = (leak_v, signal_v)[which]
            lanes = pl.ds(cuts[i] * LANES, (cuts[i + 1] - cuts[i]) * LANES)
            return pltpu.make_async_copy(
                source.at[:, :, lanes], target.at[:, :, lanes], sems.at[2 * i + which]
            )

        for i in range(len(cuts) - 1):
            fetch(0, i).start()
            fetch(1, i).start()

        def each(begin, end, act):
            lax.fori_loop(begin, end, lambda p, x: (act(p), x)[1], 0)

        barrier = pltpu.get_barrier_semaphore()

        def greet(p):
            pl.semaphore_signal(barrier, inc=1, device_id={"span": p}, device_id_type=MESH)

        def arrived(p):
            pl.semaphore_signal(ready, inc=1, device_id={"span": p}, device_id_type=MESH)

        each(me + 1, n, greet)

        @pl.when(~first)
        def _():
            pl.semaphore_wait(barrier, me)

        each(0, me, arrived)

        def spread(target, u, value):
            for s in range(SUBS):
                target[u, pl.ds(s * pitch, steps), :] = value[s * steps:(s + 1) * steps]

        def at(ref, u, k):
            return ref[u, pl.ds(k, SUBS, stride=pitch), :]

        place = lax.broadcasted_iota(jnp.int32, (SUBS, LANES), 0)

        def from_before(x, d, fill):
            return jnp.where(place < d, fill, pltpu.roll(x, d, 0))

        def from_after(x, d, fill):
            return jnp.where(place >= SUBS - d, fill, pltpu.roll(x, SUBS - d, 0))

        rate = -math.log2(math.e) / total

        def leftward(u):
            b, lanes = u % batch, pl.ds(u // batch * LANES, LANES)
            spread(keep_s, u, jnp.exp2(leak_v[b, :, lanes] * rate))
            spread(push_s, u, signal_v[b, :, lanes].astype(jnp.float32))
            q, g = at(keep_s, u, 0), at(push_s, u, 0)
            for k in range(1, steps):
                g = g + q * at(push_s, u, k)
                q = q * at(keep_s, u, k)
            local_s[u, 1] = g
            local_s[u, 2] = q
            d = 1
            while d < SUBS:
                g = g + q * pltpu.roll(g, SUBS - d, 0)
                q = q * pltpu.roll(q, SUBS - d, 0)
                d *= 2
            left_s[u:u + 1] = g[:1]

        for i in range(len(cuts) - 1):
            fetch(0, i).wait()
            fetch(1, i).wait()
            for u in range(cuts[i] * batch, cuts[i + 1] * batch):
                leftward(u)
            if cuts[i + 1] * batch == head:
                @pl.when(edge)
                def _():
                    left(sems, me, 0, 0, head).start()

        @pl.when(edge)
        def _():
            left(sems, me, 0, head, units - head, True).start()

        gates = pltpu.make_async_copy(gate_hbm, gate_v, sems.at[n])
        gates.start()

        def rightward(t, carry):
            for i in range(per * batch):
                u = t * (per * batch) + i
                f = at(push_s, u, 0)
                for k in range(1, steps):
                    f = at(keep_s, u, k) * f + at(push_s, u, k)
                g, q = local_s[u, 1], local_s[u, 2]
                a = q
                d = 1
                while d < SUBS:
                    f = f + q * from_before(f, d, 0.0)
                    g = g + a * from_after(g, d, 0.0)
                    q = q * from_before(q, d, 1.0)
                    a = a * from_after(a, d, 1.0)
                    d *= 2
                local_s[u, 0] = f
                local_s[u, 1] = g
                local_s[u, 2] = q
                local_s[u, 3] = a
                right_s[pl.ds(u, 1), :] = f[SUBS - 1:]
                right_s[pl.ds(units + u, 1), :] = q[SUBS - 1:]
                left_s[pl.ds(units + u, 1), :] = a[:1]
            return carry

        lax.fori_loop(0, trips, rightward, 0)

        @pl.when(edge)
        def _():
            each(1, me, lambda p: left(sems, me, p, 0, units).start())

        @pl.when(~edge)
        def _():
            each(0, me, lambda p: left(sems, me, p, 0, 2 * units).start())

        scale = total ** (-0.5)
        gates.wait()

        def second(t, carry):
            for i in range(per * batch):
                u = t * (per * batch) + i
                lanes = pl.ds(pl.multiple_of((t * per + i // batch) * LANES, LANES), LANES)
                x = gate_v[i % batch, :, lanes].astype(jnp.float32)
                spread(silu_s, u, (x * scale) / (1.0 + jnp.exp(-x)))
            for i in range(per * batch):
                u = t * (per * batch) + i
                f = from_before(local_s[u, 0], 1, 0.0)
                a = from_before(local_s[u, 2], 1, 1.0)
                for k in range(steps):
                    keep = at(keep_s, u, k)
                    f = keep * f + at(push_s, u, k)
                    a = a * keep
                    w_s[u, pl.ds(k, SUBS, stride=pitch), :] = f
                    u_s[u, pl.ds(k, SUBS, stride=pitch), :] = a * at(silu_s, u, k)
                g = from_after(local_s[u, 1], 1, 0.0)
                a = from_after(local_s[u, 3], 1, 1.0)
                for k in reversed(range(steps)):
                    keep, silu = at(keep_s, u, k), at(silu_s, u, k)
                    g = keep * g + at(push_s, u, k)
                    a = a * keep
                    w_s[u, pl.ds(k, SUBS, stride=pitch), :] = (at(w_s, u, k) + g) * silu
                    v_s[u, pl.ds(k, SUBS, stride=pitch), :] = a * silu
            return carry

        lax.fori_loop(0, trips, second, 0)

        @pl.when(~edge)
        def _():
            pl.semaphore_wait(ready, n - 1 - me)

        @pl.when(first)
        def _():
            each(1, n, lambda p: right(sems, me, p, units).start())

        @pl.when(~first)
        def _():
            each(me + 1, n, lambda p: right(sems, me, p, 2 * units).start())

        @pl.when(~first)
        def _():
            def join(i, state):
                s, q = state
                j = me - i
                right(sems, j, me, 2 * units).wait_recv()
                return s + q * right_r[j, :units], q * right_r[j, units:]

            s, q = lax.fori_loop(1, me, join, (zero, zero + 1.0))
            right(sems, 0, me, units).wait_recv()
            ahead_s[...] = s + q * right_r[0, :units]

            def entering(t, carry):
                for i in range(per * batch):
                    u = t * (per * batch) + i
                    ahead = ahead_s[pl.ds(u, 1), :]
                    for s in range(SUBS):
                        rows = pl.ds(s * pitch, steps)
                        w_s[u, rows, :] = w_s[u, rows, :] + u_s[u, rows, :] * ahead
                return carry

            lax.fori_loop(0, trips, entering, 0)

        @pl.when(edge)
        def _():
            left(sems, me, 0, 0, head).wait_send()
            left(sems, me, 0, head, units - head, True).wait_send()
            each(1, me, lambda p: left(sems, me, p, 0, units).wait_send())

        @pl.when(~edge)
        def _():
            each(0, me, lambda p: left(sems, me, p, 0, 2 * units).wait_send())

        @pl.when(first)
        def _():
            each(1, n, lambda p: right(sems, me, p, units).wait_send())

        @pl.when(~first)
        def _():
            each(me + 1, n, lambda p: right(sems, me, p, 2 * units).wait_send())

    pl.run_scoped(begin, pltpu.SemaphoreType.DMA((max(2 * len(cuts) - 2, n + 1),)))

    def join(j, state):
        s, q = state
        left(recv, j, me, 0, 2 * units).wait_recv()
        return s + q * left_r[j, :units], q * left_r[j, units:]

    near, far = lax.fori_loop(me + 1, n - 1, join, (zero, zero + 1.0))

    def behind(begin, end):
        behind_s[begin:end] = near[begin:end] + far[begin:end] * left_r[n - 1, begin:end]

    def leave(begin, end):
        for u in range(begin, end):
            b, lanes = u % batch, pl.ds(u // batch * LANES, LANES)
            state = behind_s[u:u + 1]
            for s in range(SUBS):
                rows = pl.ds(s * pitch, steps)
                out_ref[b, pl.ds(s * steps, steps), lanes] = (
                    w_s[u, rows, :] + v_s[u, rows, :] * state
                ).astype(out_ref.dtype)

    @pl.when(edge)
    def _():
        behind_s[...] = zero

    @pl.when(~first & ~edge)
    def _():
        left(recv, n - 1, me, 0, units).wait_recv()
        behind(0, units)

    @pl.when(first)
    def _():
        left(recv, n - 1, 0, 0, head).wait_recv()
        behind(0, head)

    leave(0, head)

    @pl.when(first)
    def _():
        left(recv, n - 1, 0, head, units - head, True).wait_recv()
        behind(head, units)

    leave(head, units)


def body(leak_rate, signal_in, gate_in):
    n = lax.axis_size("span")
    batch, length, channels = leak_rate.shape
    tiles = channels // LANES
    cuts = sorted({0, *(-(-tiles * share // 10) for share in (4, 7, 9, 10))})
    per = 2 if tiles % 2 == 0 else 1
    units = tiles * batch
    pitch = length // SUBS + 4
    hbm = pl.BlockSpec(memory_space=pl.ANY)
    f32 = jnp.float32
    spread = pltpu.VMEM((units, SUBS * pitch, LANES), f32)
    dma, regular = pltpu.SemaphoreType.DMA, pltpu.SemaphoreType.REGULAR
    return pl.pallas_call(
        functools.partial(kernel, n, length * n, batch, length, cuts, per, pitch),
        out_shape=pltpu.VMEM(leak_rate.shape, jnp.bfloat16),
        in_specs=[hbm] * 3,
        out_specs=pl.BlockSpec(memory_space=pltpu.VMEM),
        scratch_shapes=[
            pltpu.VMEM(leak_rate.shape, f32),
            pltpu.VMEM(leak_rate.shape, signal_in.dtype),
            pltpu.VMEM(leak_rate.shape, gate_in.dtype),
            spread, spread, spread, spread, spread, spread,
            pltpu.VMEM((units, 4, SUBS, LANES), f32),
            pltpu.VMEM((2 * units, LANES), f32),
            pltpu.VMEM((n, 2 * units, LANES), f32),
            pltpu.VMEM((2 * units, LANES), f32),
            pltpu.VMEM((n, 2 * units, LANES), f32),
            pltpu.VMEM((units, LANES), f32),
            pltpu.VMEM((units, LANES), f32),
            dma((n,)), regular,
        ],
        compiler_params=pltpu.CompilerParams(collective_id=0, has_side_effects=True),
    )(leak_rate, signal_in, gate_in)


def solution(mesh):
    spec = P("copy", "span", "cols")
    return jax.shard_map(body, mesh=mesh, in_specs=(spec,) * 3, out_specs=spec, check_vma=False)
```

```python
import functools
import math

import jax
import jax.numpy as jnp
from jax import lax
from jax.experimental import pallas as pl
from jax.experimental.pallas import tpu as pltpu
from jax.sharding import PartitionSpec as P

LANES = 128
SUBS = 8
MESH = pl.DeviceIdType.MESH


def kernel(
    n, total, batch, length, cuts, per, pitch,
    leak_hbm, signal_hbm, gate_hbm, out_ref,
    leak_v, signal_v, gate_v, keep_s, push_s, silu_s, w_s, u_s, v_s, local_s,
    left_s, left_r, right_s, right_r, ahead_s, behind_s,
):
    def whole(recv, ready):
        me = lax.axis_index("span")
        first, edge = me == 0, me == n - 1
        steps = length // SUBS
        tiles = cuts[-1]
        units = tiles * batch
        head = cuts[len(cuts) // 2] * batch
        trips = tiles // per

        def left(sems, source, p, start, size, second=False):
            return pltpu.make_async_remote_copy(
                src_ref=left_s.at[pl.ds(start, size)],
                dst_ref=left_r.at[source, pl.ds(start, size)],
                send_sem=sems.at[source if second else p],
                recv_sem=recv.at[p if second else source],
                device_id={"span": p},
                device_id_type=MESH,
            )

        def right(sems, source, p, size):
            return pltpu.make_async_remote_copy(
                src_ref=right_s.at[pl.ds(0, size)],
                dst_ref=right_r.at[source, pl.ds(0, size)],
                send_sem=sems.at[p],
                recv_sem=recv.at[source],
                device_id={"span": p},
                device_id_type=MESH,
            )

        zero = jnp.zeros((units, LANES), jnp.float32)

        def begin(sems):
            def fetch(which, i):
                source = (leak_hbm, signal_hbm)[which]
                target = (leak_v, signal_v)[which]
                lanes = pl.ds(cuts[i] * LANES, (cuts[i + 1] - cuts[i]) * LANES)
                return pltpu.make_async_copy(
                    source.at[:, :, lanes], target.at[:, :, lanes], sems.at[2 * i + which]
                )

            for i in range(len(cuts) - 1):
                fetch(0, i).start()
                fetch(1, i).start()

            def each(begin, end, act):
                lax.fori_loop(begin, end, lambda p, x: (act(p), x)[1], 0)

            barrier = pltpu.get_barrier_semaphore()

            def greet(p):
                pl.semaphore_signal(barrier, inc=1, device_id={"span": p}, device_id_type=MESH)

            def arrived(p):
                pl.semaphore_signal(ready, inc=1, device_id={"span": p}, device_id_type=MESH)

            each(me + 1, n, greet)

            @pl.when(~first)
            def _():
                pl.semaphore_wait(barrier, me)

            each(0, me, arrived)

            def spread(target, u, value):
                for s in range(SUBS):
                    target[u, pl.ds(s * pitch, steps), :] = value[s * steps:(s + 1) * steps]

            def at(ref, u, k):
                return ref[u, pl.ds(k, SUBS, stride=pitch), :]

            place = lax.broadcasted_iota(jnp.int32, (SUBS, LANES), 0)

            def from_before(x, d, fill):
                return jnp.where(place < d, fill, pltpu.roll(x, d, 0))

            def from_after(x, d, fill):
                return jnp.where(place >= SUBS - d, fill, pltpu.roll(x, SUBS - d, 0))

            rate = -math.log2(math.e) / total

            def leftward(u):
                b, lanes = u % batch, pl.ds(u // batch * LANES, LANES)
                spread(keep_s, u, jnp.exp2(leak_v[b, :, lanes] * rate))
                spread(push_s, u, signal_v[b, :, lanes].astype(jnp.float32))
                q, g = at(keep_s, u, 0), at(push_s, u, 0)
                for k in range(1, steps):
                    g = g + q * at(push_s, u, k)
                    q = q * at(keep_s, u, k)
                local_s[u, 1] = g
                local_s[u, 2] = q
                d = 1
                while d < SUBS:
                    g = g + q * pltpu.roll(g, SUBS - d, 0)
                    q = q * pltpu.roll(q, SUBS - d, 0)
                    d *= 2
                left_s[u:u + 1] = g[:1]

            for i in range(len(cuts) - 1):
                fetch(0, i).wait()
                fetch(1, i).wait()
                for u in range(cuts[i] * batch, cuts[i + 1] * batch):
                    leftward(u)
                if cuts[i + 1] * batch == head:
                    @pl.when(edge)
                    def _():
                        left(sems, me, 0, 0, head).start()

            @pl.when(edge)
            def _():
                left(sems, me, 0, head, units - head, True).start()

            gates = pltpu.make_async_copy(gate_hbm, gate_v, sems.at[n])
            gates.start()

            def rightward(t, carry):
                for i in range(per * batch):
                    u = t * (per * batch) + i
                    f = at(push_s, u, 0)
                    for k in range(1, steps):
                        f = at(keep_s, u, k) * f + at(push_s, u, k)
                    g, q = local_s[u, 1], local_s[u, 2]
                    a = q
                    d = 1
                    while d < SUBS:
                        f = f + q * from_before(f, d, 0.0)
                        g = g + a * from_after(g, d, 0.0)
                        q = q * from_before(q, d, 1.0)
                        a = a * from_after(a, d, 1.0)
                        d *= 2
                    local_s[u, 0] = f
                    local_s[u, 1] = g
                    local_s[u, 2] = q
                    local_s[u, 3] = a
                    right_s[pl.ds(u, 1), :] = f[SUBS - 1:]
                    right_s[pl.ds(units + u, 1), :] = q[SUBS - 1:]
                    left_s[pl.ds(units + u, 1), :] = a[:1]
                return carry

            lax.fori_loop(0, trips, rightward, 0)

            @pl.when(edge)
            def _():
                each(1, me, lambda p: left(sems, me, p, 0, units).start())

            @pl.when(~edge)
            def _():
                each(0, me, lambda p: left(sems, me, p, 0, 2 * units).start())

            scale = total ** (-0.5)
            gates.wait()

            def second(t, carry):
                for i in range(per * batch):
                    u = t * (per * batch) + i
                    lanes = pl.ds(pl.multiple_of((t * per + i // batch) * LANES, LANES), LANES)
                    x = gate_v[i % batch, :, lanes].astype(jnp.float32)
                    spread(silu_s, u, (x * scale) / (1.0 + jnp.exp(-x)))
                for i in range(per * batch):
                    u = t * (per * batch) + i
                    f = from_before(local_s[u, 0], 1, 0.0)
                    a = from_before(local_s[u, 2], 1, 1.0)
                    for k in range(steps):
                        keep = at(keep_s, u, k)
                        f = keep * f + at(push_s, u, k)
                        a = a * keep
                        w_s[u, pl.ds(k, SUBS, stride=pitch), :] = f
                        u_s[u, pl.ds(k, SUBS, stride=pitch), :] = a * at(silu_s, u, k)
                    g = from_after(local_s[u, 1], 1, 0.0)
                    a = from_after(local_s[u, 3], 1, 1.0)
                    for k in reversed(range(steps)):
                        keep, silu = at(keep_s, u, k), at(silu_s, u, k)
                        g = keep * g + at(push_s, u, k)
                        a = a * keep
                        w_s[u, pl.ds(k, SUBS, stride=pitch), :] = (at(w_s, u, k) + g) * silu
                        v_s[u, pl.ds(k, SUBS, stride=pitch), :] = a * silu
                return carry

            lax.fori_loop(0, trips, second, 0)

            @pl.when(~edge)
            def _():
                pl.semaphore_wait(ready, n - 1 - me)

            @pl.when(first)
            def _():
                each(1, n, lambda p: right(sems, me, p, units).start())

            @pl.when(~first)
            def _():
                each(me + 1, n, lambda p: right(sems, me, p, 2 * units).start())

            @pl.when(~first)
            def _():
                def join(i, state):
                    s, q = state
                    j = me - i
                    right(sems, j, me, 2 * units).wait_recv()
                    return s + q * right_r[j, :units], q * right_r[j, units:]

                s, q = lax.fori_loop(1, me, join, (zero, zero + 1.0))
                right(sems, 0, me, units).wait_recv()
                ahead_s[...] = s + q * right_r[0, :units]

                def entering(t, carry):
                    for i in range(per * batch):
                        u = t * (per * batch) + i
                        ahead = ahead_s[pl.ds(u, 1), :]
                        for s in range(SUBS):
                            rows = pl.ds(s * pitch, steps)
                            w_s[u, rows, :] = w_s[u, rows, :] + u_s[u, rows, :] * ahead
                    return carry

                lax.fori_loop(0, trips, entering, 0)

            @pl.when(edge)
            def _():
                left(sems, me, 0, 0, head).wait_send()
                left(sems, me, 0, head, units - head, True).wait_send()
                each(1, me, lambda p: left(sems, me, p, 0, units).wait_send())

            @pl.when(~edge)
            def _():
                each(0, me, lambda p: left(sems, me, p, 0, 2 * units).wait_send())

            @pl.when(first)
            def _():
                each(1, n, lambda p: right(sems, me, p, units).wait_send())

            @pl.when(~first)
            def _():
                each(me + 1, n, lambda p: right(sems, me, p, 2 * units).wait_send())

        pl.run_scoped(begin, pltpu.SemaphoreType.DMA((max(2 * len(cuts) - 2, n + 1),)))

        def join(j, state):
            s, q = state
            left(recv, j, me, 0, 2 * units).wait_recv()
            return s + q * left_r[j, :units], q * left_r[j, units:]

        near, far = lax.fori_loop(me + 1, n - 1, join, (zero, zero + 1.0))

        def behind(begin, end):
            behind_s[begin:end] = near[begin:end] + far[begin:end] * left_r[n - 1, begin:end]

        def leave(begin, end):
            for u in range(begin, end):
                b, lanes = u % batch, pl.ds(u // batch * LANES, LANES)
                state = behind_s[u:u + 1]
                for s in range(SUBS):
                    rows = pl.ds(s * pitch, steps)
                    out_ref[b, pl.ds(s * steps, steps), lanes] = (
                        w_s[u, rows, :] + v_s[u, rows, :] * state
                    ).astype(out_ref.dtype)

        @pl.when(edge)
        def _():
            behind_s[...] = zero

        @pl.when(~first & ~edge)
        def _():
            left(recv, n - 1, me, 0, units).wait_recv()
            behind(0, units)

        @pl.when(first)
        def _():
            left(recv, n - 1, 0, 0, head).wait_recv()
            behind(0, head)

        leave(0, head)

        @pl.when(first)
        def _():
            left(recv, n - 1, 0, head, units - head, True).wait_recv()
            behind(head, units)

        leave(head, units)

    pl.run_scoped(whole, pltpu.SemaphoreType.DMA((n,)), pltpu.SemaphoreType.REGULAR)


def body(leak_rate, signal_in, gate_in):
    n = lax.axis_size("span")
    batch, length, channels = leak_rate.shape
    tiles = channels // LANES
    cuts = sorted({0, *(-(-tiles * share // 10) for share in (4, 7, 9, 10))})
    per = 2 if tiles % 2 == 0 else 1
    units = tiles * batch
    pitch = length // SUBS + 4
    hbm = pl.BlockSpec(memory_space=pl.ANY)
    f32 = jnp.float32
    spread = pltpu.VMEM((units, SUBS * pitch, LANES), f32)
    return pl.pallas_call(
        functools.partial(kernel, n, length * n, batch, length, cuts, per, pitch),
        out_shape=pltpu.VMEM(leak_rate.shape, jnp.bfloat16),
        in_specs=[hbm] * 3,
        out_specs=pl.BlockSpec(memory_space=pltpu.VMEM),
        scratch_shapes=[
            pltpu.VMEM(leak_rate.shape, f32),
            pltpu.VMEM(leak_rate.shape, signal_in.dtype),
            pltpu.VMEM(leak_rate.shape, gate_in.dtype),
            spread, spread, spread, spread, spread, spread,
            pltpu.VMEM((units, 4, SUBS, LANES), f32),
            pltpu.VMEM((2 * units, LANES), f32),
            pltpu.VMEM((n, 2 * units, LANES), f32),
            pltpu.VMEM((2 * units, LANES), f32),
            pltpu.VMEM((n, 2 * units, LANES), f32),
            pltpu.VMEM((units, LANES), f32),
            pltpu.VMEM((units, LANES), f32),
        ],
        compiler_params=pltpu.CompilerParams(collective_id=0, has_side_effects=True),
    )(leak_rate, signal_in, gate_in)


def solution(mesh):
    spec = P("copy", "span", "cols")
    return jax.shard_map(body, mesh=mesh, in_specs=(spec,) * 3, out_specs=spec, check_vma=False)
```

```python
import functools
import math

import jax
import jax.numpy as jnp
from jax import lax
from jax.experimental import pallas as pl
from jax.experimental.pallas import tpu as pltpu
from jax.sharding import PartitionSpec as P

LANES = 128
SUBS = 8
MESH = pl.DeviceIdType.MESH


def kernel(
    n, total, batch, length, cuts, per, pitch,
    leak_hbm, signal_hbm, gate_hbm, out_ref, base_ref, slope_ref, state_ref,
    leak_v, signal_v, gate_v, keep_s, push_s, silu_s, w_s, u_s, v_s, local_s,
    left_s, left_r, right_s, right_r, ahead_s, behind_s,
):
    def whole(recv, ready):
        me = lax.axis_index("span")
        first, edge = me == 0, me == n - 1
        steps = length // SUBS
        tiles = cuts[-1]
        units = tiles * batch
        head = cuts[len(cuts) // 2] * batch
        trips = tiles // per

        def left(sems, source, p, start, size, second=False):
            return pltpu.make_async_remote_copy(
                src_ref=left_s.at[pl.ds(start, size)],
                dst_ref=left_r.at[source, pl.ds(start, size)],
                send_sem=sems.at[source if second else p],
                recv_sem=recv.at[p if second else source],
                device_id={"span": p},
                device_id_type=MESH,
            )

        def right(sems, source, p, size):
            return pltpu.make_async_remote_copy(
                src_ref=right_s.at[pl.ds(0, size)],
                dst_ref=right_r.at[source, pl.ds(0, size)],
                send_sem=sems.at[p],
                recv_sem=recv.at[source],
                device_id={"span": p},
                device_id_type=MESH,
            )

        zero = jnp.zeros((units, LANES), jnp.float32)

        def begin(sems):
            def fetch(which, i):
                source = (leak_hbm, signal_hbm)[which]
                target = (leak_v, signal_v)[which]
                lanes = pl.ds(cuts[i] * LANES, (cuts[i + 1] - cuts[i]) * LANES)
                return pltpu.make_async_copy(
                    source.at[:, :, lanes], target.at[:, :, lanes], sems.at[2 * i + which]
                )

            for i in range(len(cuts) - 1):
                fetch(0, i).start()
                fetch(1, i).start()

            def each(begin, end, act):
                lax.fori_loop(begin, end, lambda p, x: (act(p), x)[1], 0)

            barrier = pltpu.get_barrier_semaphore()

            def greet(p):
                pl.semaphore_signal(barrier, inc=1, device_id={"span": p}, device_id_type=MESH)

            def arrived(p):
                pl.semaphore_signal(ready, inc=1, device_id={"span": p}, device_id_type=MESH)

            each(me + 1, n, greet)

            @pl.when(~first)
            def _():
                pl.semaphore_wait(barrier, me)

            each(0, me, arrived)

            def spread(target, u, value):
                for s in range(SUBS):
                    target[u, pl.ds(s * pitch, steps), :] = value[s * steps:(s + 1) * steps]

            def at(ref, u, k):
                return ref[u, pl.ds(k, SUBS, stride=pitch), :]

            place = lax.broadcasted_iota(jnp.int32, (SUBS, LANES), 0)

            def from_before(x, d, fill):
                return jnp.where(place < d, fill, pltpu.roll(x, d, 0))

            def from_after(x, d, fill):
                return jnp.where(place >= SUBS - d, fill, pltpu.roll(x, SUBS - d, 0))

            rate = -math.log2(math.e) / total

            def sweep(u, pieces):
                b, lanes = u % batch, pl.ds(u // batch * LANES, LANES)
                spread(keep_s, u, jnp.exp2(leak_v[b, :, lanes] * rate))
                spread(push_s, u, signal_v[b, :, lanes].astype(jnp.float32))
                size = steps // pieces
                g, q = [], []
                for i in range(pieces):
                    g.append(at(push_s, u, i * size))
                    q.append(at(keep_s, u, i * size))
                for k in range(1, size):
                    for i in range(pieces):
                        g[i] = g[i] + q[i] * at(push_s, u, i * size + k)
                        q[i] = q[i] * at(keep_s, u, i * size + k)
                for i in range(1, pieces):
                    g[0], q[0] = g[0] + q[0] * g[i], q[0] * q[i]
                local_s[u, 1] = g[0]
                local_s[u, 2] = q[0]
                return u, g[0], q[0]

            def total_of(u, g, q):
                d = 1
                while d < SUBS:
                    g = g + q * pltpu.roll(g, SUBS - d, 0)
                    q = q * pltpu.roll(q, SUBS - d, 0)
                    d *= 2
                left_s[u:u + 1] = g[:1]

            swept = []
            for i in range(len(cuts) - 1):
                fetch(0, i).wait()
                fetch(1, i).wait()
                here = range(cuts[i] * batch, cuts[i + 1] * batch)
                final = here.stop == units
                swept += [sweep(u, 2 if final else 1) for u in here]
                if final or here.stop == head:
                    for one in swept:
                        total_of(*one)
                    swept = []
                if here.stop == head:
                    @pl.when(edge)
                    def _():
                        left(sems, me, 0, 0, head).start()

            @pl.when(edge)
            def _():
                left(sems, me, 0, head, units - head, True).start()

            gates = pltpu.make_async_copy(gate_hbm, gate_v, sems.at[n])
            gates.start()

            def rightward(t, carry):
                for i in range(per * batch):
                    u = t * (per * batch) + i
                    f = at(push_s, u, 0)
                    for k in range(1, steps):
                        f = at(keep_s, u, k) * f + at(push_s, u, k)
                    g, q = local_s[u, 1], local_s[u, 2]
                    a = q
                    d = 1
                    while d < SUBS:
                        f = f + q * from_before(f, d, 0.0)
                        g = g + a * from_after(g, d, 0.0)
                        q = q * from_before(q, d, 1.0)
                        a = a * from_after(a, d, 1.0)
                        d *= 2
                    local_s[u, 0] = f
                    local_s[u, 1] = g
                    local_s[u, 2] = q
                    local_s[u, 3] = a
                    right_s[pl.ds(u, 1), :] = f[SUBS - 1:]
                    right_s[pl.ds(units + u, 1), :] = q[SUBS - 1:]
                    left_s[pl.ds(units + u, 1), :] = a[:1]
                return carry

            lax.fori_loop(0, trips, rightward, 0)

            @pl.when(edge)
            def _():
                each(1, me, lambda p: left(sems, me, p, 0, units).start())

            @pl.when(~edge)
            def _():
                each(0, me, lambda p: left(sems, me, p, 0, 2 * units).start())

            scale = total ** (-0.5)
            gates.wait()

            def second(t, carry):
                for i in range(per * batch):
                    u = t * (per * batch) + i
                    lanes = pl.ds(pl.multiple_of((t * per + i // batch) * LANES, LANES), LANES)
                    x = gate_v[i % batch, :, lanes].astype(jnp.float32)
                    spread(silu_s, u, (x * scale) / (1.0 + jnp.exp(-x)))
                for i in range(per * batch):
                    u = t * (per * batch) + i
                    f = from_before(local_s[u, 0], 1, 0.0)
                    a = from_before(local_s[u, 2], 1, 1.0)
                    for k in range(steps):
                        keep = at(keep_s, u, k)
                        f = keep * f + at(push_s, u, k)
                        a = a * keep
                        w_s[u, pl.ds(k, SUBS, stride=pitch), :] = f
                        u_s[u, pl.ds(k, SUBS, stride=pitch), :] = a * at(silu_s, u, k)
                    g = from_after(local_s[u, 1], 1, 0.0)
                    a = from_after(local_s[u, 3], 1, 1.0)
                    for k in reversed(range(steps)):
                        keep, silu = at(keep_s, u, k), at(silu_s, u, k)
                        g = keep * g + at(push_s, u, k)
                        a = a * keep
                        w_s[u, pl.ds(k, SUBS, stride=pitch), :] = (at(w_s, u, k) + g) * silu
                        v_s[u, pl.ds(k, SUBS, stride=pitch), :] = a * silu
                return carry

            lax.fori_loop(0, trips, second, 0)

            @pl.when(~edge)
            def _():
                pl.semaphore_wait(ready, n - 1 - me)

            @pl.when(first)
            def _():
                each(1, n, lambda p: right(sems, me, p, units).start())

            @pl.when(~first)
            def _():
                each(me + 1, n, lambda p: right(sems, me, p, 2 * units).start())

            @pl.when(~first)
            def _():
                def join(i, state):
                    s, q = state
                    j = me - i
                    right(sems, j, me, 2 * units).wait_recv()
                    return s + q * right_r[j, :units], q * right_r[j, units:]

                s, q = lax.fori_loop(1, me, join, (zero, zero + 1.0))
                right(sems, 0, me, units).wait_recv()
                ahead_s[...] = s + q * right_r[0, :units]

                def entering(t, carry):
                    for i in range(per * batch):
                        u = t * (per * batch) + i
                        ahead = ahead_s[pl.ds(u, 1), :]
                        for s in range(SUBS):
                            rows = pl.ds(s * pitch, steps)
                            w_s[u, rows, :] = w_s[u, rows, :] + u_s[u, rows, :] * ahead
                    return carry

                lax.fori_loop(0, trips, entering, 0)

            @pl.when(edge)
            def _():
                left(sems, me, 0, 0, head).wait_send()
                left(sems, me, 0, head, units - head, True).wait_send()
                each(1, me, lambda p: left(sems, me, p, 0, units).wait_send())

            @pl.when(~edge)
            def _():
                each(0, me, lambda p: left(sems, me, p, 0, 2 * units).wait_send())

            @pl.when(first)
            def _():
                each(1, n, lambda p: right(sems, me, p, units).wait_send())

            @pl.when(~first)
            def _():
                each(me + 1, n, lambda p: right(sems, me, p, 2 * units).wait_send())

        pl.run_scoped(begin, pltpu.SemaphoreType.DMA((max(2 * len(cuts) - 2, n + 1),)))

        for u in range(head, units):
            base_ref[u - head] = w_s[u]
            slope_ref[u - head] = v_s[u]

        def join(j, state):
            s, q = state
            left(recv, j, me, 0, 2 * units).wait_recv()
            return s + q * left_r[j, :units], q * left_r[j, units:]

        near, far = lax.fori_loop(me + 1, n - 1, join, (zero, zero + 1.0))

        def behind(ref, begin, end):
            ref[0:end - begin] = (
                near[begin:end] + far[begin:end] * left_r[n - 1, begin:end]
            )

        @pl.when(edge)
        def _():
            behind_s[...] = zero
            state_ref[...] = zero[head:]

        @pl.when(~first & ~edge)
        def _():
            left(recv, n - 1, me, 0, units).wait_recv()
            behind(behind_s, 0, head)
            behind(state_ref, head, units)

        @pl.when(first)
        def _():
            left(recv, n - 1, 0, 0, head).wait_recv()
            behind(behind_s, 0, head)

        for u in range(head):
            b, lanes = u % batch, pl.ds(u // batch * LANES, LANES)
            state = behind_s[u:u + 1]
            for s in range(SUBS):
                rows = pl.ds(s * pitch, steps)
                out_ref[b, pl.ds(s * steps, steps), lanes] = (
                    w_s[u, rows, :] + v_s[u, rows, :] * state
                ).astype(out_ref.dtype)

        @pl.when(first)
        def _():
            left(recv, n - 1, 0, head, units - head, True).wait_recv()
            behind(state_ref, head, units)

    pl.run_scoped(whole, pltpu.SemaphoreType.DMA((n,)), pltpu.SemaphoreType.REGULAR)


def write(
    batch, steps, pitch, done_ref, base_ref, slope_ref, state_ref, out_hbm, tail_v
):
    done, channels = done_ref.shape[2], out_hbm.shape[2]

    def put(sem):
        early = pltpu.make_async_copy(done_ref, out_hbm.at[:, :, pl.ds(0, done)], sem.at[0])
        late = pltpu.make_async_copy(
            tail_v, out_hbm.at[:, :, pl.ds(done, channels - done)], sem.at[1]
        )
        early.start()
        for u in range(base_ref.shape[0]):
            b, lanes = u % batch, pl.ds(u // batch * LANES, LANES)
            state = state_ref[u:u + 1]
            for s in range(SUBS):
                rows = pl.ds(s * pitch, steps)
                tail_v[b, pl.ds(s * steps, steps), lanes] = (
                    base_ref[u, rows, :] + slope_ref[u, rows, :] * state
                ).astype(tail_v.dtype)
        late.start()
        early.wait()
        late.wait()

    pl.run_scoped(put, pltpu.SemaphoreType.DMA((2,)))


def body(leak_rate, signal_in, gate_in):
    n = lax.axis_size("span")
    batch, length, channels = leak_rate.shape
    tiles = channels // LANES
    cuts = sorted({0, *(-(-tiles * share // 10) for share in (4, 7, 9, 10))})
    per = 2 if tiles % 2 == 0 else 1
    units = tiles * batch
    pitch = length // SUBS + 4
    hbm = pl.BlockSpec(memory_space=pl.ANY)
    f32 = jnp.float32
    spread = pltpu.VMEM((units, SUBS * pitch, LANES), f32)
    head = cuts[len(cuts) // 2]
    late = (tiles - head) * batch
    vmem = pl.BlockSpec(memory_space=pltpu.VMEM)
    bf16 = jnp.bfloat16
    parts = pl.pallas_call(
        functools.partial(kernel, n, length * n, batch, length, cuts, per, pitch),
        out_shape=[
            pltpu.VMEM((batch, length, head * LANES), bf16),
            pltpu.VMEM((late, SUBS * pitch, LANES), f32),
            pltpu.VMEM((late, SUBS * pitch, LANES), f32),
            pltpu.VMEM((late, LANES), f32),
        ],
        in_specs=[hbm] * 3,
        out_specs=[vmem] * 4,
        scratch_shapes=[
            pltpu.VMEM(leak_rate.shape, f32),
            pltpu.VMEM(leak_rate.shape, signal_in.dtype),
            pltpu.VMEM(leak_rate.shape, gate_in.dtype),
            spread, spread, spread, spread, spread, spread,
            pltpu.VMEM((units, 4, SUBS, LANES), f32),
            pltpu.VMEM((2 * units, LANES), f32),
            pltpu.VMEM((n, 2 * units, LANES), f32),
            pltpu.VMEM((2 * units, LANES), f32),
            pltpu.VMEM((n, 2 * units, LANES), f32),
            pltpu.VMEM((units, LANES), f32),
            pltpu.VMEM((units, LANES), f32),
        ],
        compiler_params=pltpu.CompilerParams(collective_id=0, has_side_effects=True),
    )(leak_rate, signal_in, gate_in)
    return pl.pallas_call(
        functools.partial(write, batch, length // SUBS, pitch),
        out_shape=jax.ShapeDtypeStruct(leak_rate.shape, bf16),
        in_specs=[vmem] * 4,
        out_specs=hbm,
        scratch_shapes=[pltpu.VMEM((batch, length, channels - head * LANES), bf16)],
        compiler_params=pltpu.CompilerParams(vmem_limit_bytes=4 << 20),
    )(*parts)


def solution(mesh):
    spec = P("copy", "span", "cols")
    return jax.shard_map(body, mesh=mesh, in_specs=(spec,) * 3, out_specs=spec, check_vma=False)
```

```python
import functools
import math

import jax
import jax.numpy as jnp
from jax import lax
from jax.experimental import pallas as pl
from jax.experimental.pallas import tpu as pltpu
from jax.sharding import PartitionSpec as P

LANES = 128
SUBS = 8
MESH = pl.DeviceIdType.MESH


def kernel(
    n, total, batch, length, cuts, per, pitch,
    leak_hbm, signal_hbm, gate_hbm, out_ref, base_ref, slope_ref, state_ref,
    leak_v, signal_v, gate_v, keep_s, push_s, silu_s, w_s, u_s, v_s, local_s,
    left_s, left_r, right_s, right_r, ahead_s, behind_s,
):
    def whole(sems, recv, ready):
        steps = length // SUBS
        tiles = cuts[-1]
        units = tiles * batch
        head = cuts[1] * batch
        trips = tiles // per

        def fetch(which, i):
            source = (leak_hbm, signal_hbm)[which]
            target = (leak_v, signal_v)[which]
            lanes = pl.ds(cuts[i] * LANES, (cuts[i + 1] - cuts[i]) * LANES)
            return pltpu.make_async_copy(
                source.at[:, :, lanes], target.at[:, :, lanes], sems.at[2 * i + which]
            )

        for i in range(len(cuts) - 1):
            fetch(0, i).start()
            fetch(1, i).start()

        me = lax.axis_index("span")
        first, edge = me == 0, me == n - 1

        def left(sems, source, p, start, size, second=False):
            return pltpu.make_async_remote_copy(
                src_ref=left_s.at[pl.ds(start, size)],
                dst_ref=left_r.at[source, pl.ds(start, size)],
                send_sem=sems.at[source if second else p],
                recv_sem=recv.at[p if second else source],
                device_id={"span": p},
                device_id_type=MESH,
            )

        def right(sems, source, p, size):
            return pltpu.make_async_remote_copy(
                src_ref=right_s.at[pl.ds(0, size)],
                dst_ref=right_r.at[source, pl.ds(0, size)],
                send_sem=sems.at[p],
                recv_sem=recv.at[source],
                device_id={"span": p},
                device_id_type=MESH,
            )

        zero = jnp.zeros((units, LANES), jnp.float32)

        def begin():
            def each(begin, end, act):
                lax.fori_loop(begin, end, lambda p, x: (act(p), x)[1], 0)

            barrier = pltpu.get_barrier_semaphore()

            def greet(p):
                pl.semaphore_signal(barrier, inc=1, device_id={"span": p}, device_id_type=MESH)

            def arrived(p):
                pl.semaphore_signal(ready, inc=1, device_id={"span": p}, device_id_type=MESH)

            each(me + 1, n, greet)

            @pl.when(~first)
            def _():
                pl.semaphore_wait(barrier, me)

            each(0, me, arrived)

            def spread(target, u, value):
                for s in range(SUBS):
                    target[u, pl.ds(s * pitch, steps), :] = value[s * steps:(s + 1) * steps]

            def at(ref, u, k):
                return ref[u, pl.ds(k, SUBS, stride=pitch), :]

            place = lax.broadcasted_iota(jnp.int32, (SUBS, LANES), 0)

            def from_before(x, d, fill):
                return jnp.where(place < d, fill, pltpu.roll(x, d, 0))

            def from_after(x, d, fill):
                return jnp.where(place >= SUBS - d, fill, pltpu.roll(x, SUBS - d, 0))

            rate = -math.log2(math.e) / total

            def sweep(u, pieces):
                b, lanes = u % batch, pl.ds(u // batch * LANES, LANES)
                spread(keep_s, u, jnp.exp2(leak_v[b, :, lanes] * rate))
                spread(push_s, u, signal_v[b, :, lanes].astype(jnp.float32))
                size = steps // pieces
                g, q = [], []
                for i in range(pieces):
                    g.append(at(push_s, u, i * size))
                    q.append(at(keep_s, u, i * size))
                for k in range(1, size):
                    for i in range(pieces):
                        g[i] = g[i] + q[i] * at(push_s, u, i * size + k)
                        q[i] = q[i] * at(keep_s, u, i * size + k)
                for i in range(1, pieces):
                    g[0], q[0] = g[0] + q[0] * g[i], q[0] * q[i]
                local_s[u, 1] = g[0]
                local_s[u, 2] = q[0]
                return u, g[0], q[0]

            def total_of(u, g, q):
                d = 1
                while d < SUBS:
                    g = g + q * pltpu.roll(g, SUBS - d, 0)
                    q = q * pltpu.roll(q, SUBS - d, 0)
                    d *= 2
                left_s[u:u + 1] = g[:1]

            swept = []
            for i in range(len(cuts) - 1):
                fetch(0, i).wait()
                fetch(1, i).wait()
                here = range(cuts[i] * batch, cuts[i + 1] * batch)
                final = here.stop == units
                now = [sweep(u, 2 if final else 1) for u in here]
                if final or here.stop == head:
                    swept, now = swept + now, []
                for one in swept:
                    total_of(*one)
                swept = now
                if here.stop == head:
                    @pl.when(edge)
                    def _():
                        left(sems, me, 0, 0, head).start()

            @pl.when(edge)
            def _():
                left(sems, me, 0, head, units - head, True).start()

            gates = pltpu.make_async_copy(gate_hbm, gate_v, sems.at[n])
            gates.start()

            def rightward(t, carry):
                for i in range(per * batch):
                    u = t * (per * batch) + i
                    f = at(push_s, u, 0)
                    for k in range(1, steps):
                        f = at(keep_s, u, k) * f + at(push_s, u, k)
                    g, q = local_s[u, 1], local_s[u, 2]
                    a = q
                    d = 1
                    while d < SUBS:
                        f = f + q * from_before(f, d, 0.0)
                        g = g + a * from_after(g, d, 0.0)
                        q = q * from_before(q, d, 1.0)
                        a = a * from_after(a, d, 1.0)
                        d *= 2
                    local_s[u, 0] = f
                    local_s[u, 1] = g
                    local_s[u, 2] = q
                    local_s[u, 3] = a
                    right_s[pl.ds(u, 1), :] = f[SUBS - 1:]
                    right_s[pl.ds(units + u, 1), :] = q[SUBS - 1:]
                    left_s[pl.ds(units + u, 1), :] = a[:1]
                return carry

            lax.fori_loop(0, trips, rightward, 0)

            @pl.when(edge)
            def _():
                each(1, me, lambda p: left(sems, me, p, 0, units).start())

            @pl.when(~edge)
            def _():
                each(0, me, lambda p: left(sems, me, p, 0, 2 * units).start())

            scale = total ** (-0.5)
            gates.wait()

            def second(t, carry):
                for i in range(per * batch):
                    u = t * (per * batch) + i
                    lanes = pl.ds(pl.multiple_of((t * per + i // batch) * LANES, LANES), LANES)
                    x = gate_v[i % batch, :, lanes].astype(jnp.float32)
                    spread(silu_s, u, (x * scale) / (1.0 + jnp.exp(-x)))
                for i in range(per * batch):
                    u = t * (per * batch) + i
                    f = from_before(local_s[u, 0], 1, 0.0)
                    a = from_before(local_s[u, 2], 1, 1.0)
                    for k in range(steps):
                        keep = at(keep_s, u, k)
                        f = keep * f + at(push_s, u, k)
                        a = a * keep
                        w_s[u, pl.ds(k, SUBS, stride=pitch), :] = f
                        u_s[u, pl.ds(k, SUBS, stride=pitch), :] = a * at(silu_s, u, k)
                    g = from_after(local_s[u, 1], 1, 0.0)
                    a = from_after(local_s[u, 3], 1, 1.0)
                    for k in reversed(range(steps)):
                        keep, silu = at(keep_s, u, k), at(silu_s, u, k)
                        g = keep * g + at(push_s, u, k)
                        a = a * keep
                        w_s[u, pl.ds(k, SUBS, stride=pitch), :] = (at(w_s, u, k) + g) * silu
                        v_s[u, pl.ds(k, SUBS, stride=pitch), :] = a * silu
                return carry

            lax.fori_loop(0, trips, second, 0)

            @pl.when(~edge)
            def _():
                pl.semaphore_wait(ready, n - 1 - me)

            @pl.when(first)
            def _():
                each(1, n, lambda p: right(sems, me, p, units).start())

            @pl.when(~first)
            def _():
                each(me + 1, n, lambda p: right(sems, me, p, 2 * units).start())

            @pl.when(~first)
            def _():
                def join(i, state):
                    s, q = state
                    j = me - i
                    right(sems, j, me, 2 * units).wait_recv()
                    return s + q * right_r[j, :units], q * right_r[j, units:]

                s, q = lax.fori_loop(1, me, join, (zero, zero + 1.0))
                right(sems, 0, me, units).wait_recv()
                ahead_s[...] = s + q * right_r[0, :units]

                def entering(t, carry):
                    for i in range(per * batch):
                        u = t * (per * batch) + i
                        ahead = ahead_s[pl.ds(u, 1), :]
                        for s in range(SUBS):
                            rows = pl.ds(s * pitch, steps)
                            w_s[u, rows, :] = w_s[u, rows, :] + u_s[u, rows, :] * ahead
                    return carry

                lax.fori_loop(0, trips, entering, 0)

            @pl.when(edge)
            def _():
                left(sems, me, 0, 0, head).wait_send()
                left(sems, me, 0, head, units - head, True).wait_send()
                each(1, me, lambda p: left(sems, me, p, 0, units).wait_send())

            @pl.when(~edge)
            def _():
                each(0, me, lambda p: left(sems, me, p, 0, 2 * units).wait_send())

            @pl.when(first)
            def _():
                each(1, n, lambda p: right(sems, me, p, units).wait_send())

            @pl.when(~first)
            def _():
                each(me + 1, n, lambda p: right(sems, me, p, 2 * units).wait_send())

        begin()

        for u in range(head, units):
            base_ref[u - head] = w_s[u]
            slope_ref[u - head] = v_s[u]

        def join(j, state):
            s, q = state
            left(recv, j, me, 0, 2 * units).wait_recv()
            return s + q * left_r[j, :units], q * left_r[j, units:]

        near, far = lax.fori_loop(me + 1, n - 1, join, (zero, zero + 1.0))

        def behind(ref, begin, end):
            ref[0:end - begin] = (
                near[begin:end] + far[begin:end] * left_r[n - 1, begin:end]
            )

        @pl.when(edge)
        def _():
            behind_s[...] = zero
            state_ref[...] = zero[head:]

        @pl.when(~first & ~edge)
        def _():
            left(recv, n - 1, me, 0, units).wait_recv()
            behind(behind_s, 0, head)
            behind(state_ref, head, units)

        @pl.when(first)
        def _():
            left(recv, n - 1, 0, 0, head).wait_recv()
            behind(behind_s, 0, head)

        for u in range(head):
            b, lanes = u % batch, pl.ds(u // batch * LANES, LANES)
            state = behind_s[u:u + 1]
            for s in range(SUBS):
                rows = pl.ds(s * pitch, steps)
                out_ref[b, pl.ds(s * steps, steps), lanes] = (
                    w_s[u, rows, :] + v_s[u, rows, :] * state
                ).astype(out_ref.dtype)

        @pl.when(first)
        def _():
            left(recv, n - 1, 0, head, units - head, True).wait_recv()
            behind(state_ref, head, units)

    pl.run_scoped(
        whole,
        pltpu.SemaphoreType.DMA((max(2 * len(cuts) - 2, n + 1),)),
        pltpu.SemaphoreType.DMA((n,)),
        pltpu.SemaphoreType.REGULAR,
    )


def write(
    batch, steps, pitch, done_ref, base_ref, slope_ref, state_ref, out_hbm, tail_v
):
    done, channels = done_ref.shape[2], out_hbm.shape[2]

    def put(sem):
        early = pltpu.make_async_copy(done_ref, out_hbm.at[:, :, pl.ds(0, done)], sem.at[0])
        late = pltpu.make_async_copy(
            tail_v, out_hbm.at[:, :, pl.ds(done, channels - done)], sem.at[1]
        )
        early.start()
        for u in range(base_ref.shape[0]):
            b, lanes = u % batch, pl.ds(u // batch * LANES, LANES)
            state = state_ref[u:u + 1]
            for s in range(SUBS):
                rows = pl.ds(s * pitch, steps)
                tail_v[b, pl.ds(s * steps, steps), lanes] = (
                    base_ref[u, rows, :] + slope_ref[u, rows, :] * state
                ).astype(tail_v.dtype)
        late.start()
        early.wait()
        late.wait()

    pl.run_scoped(put, pltpu.SemaphoreType.DMA((2,)))


def body(leak_rate, signal_in, gate_in):
    n = lax.axis_size("span")
    batch, length, channels = leak_rate.shape
    tiles = channels // LANES
    cuts = sorted({0, *(-(-tiles * share // 10) for share in (4, 7, 9, 10))})
    per = 2 if tiles % 2 == 0 else 1
    units = tiles * batch
    pitch = length // SUBS + 4
    hbm = pl.BlockSpec(memory_space=pl.ANY)
    f32 = jnp.float32
    spread = pltpu.VMEM((units, SUBS * pitch, LANES), f32)
    head = cuts[1]
    late = (tiles - head) * batch
    vmem = pl.BlockSpec(memory_space=pltpu.VMEM)
    bf16 = jnp.bfloat16
    parts = pl.pallas_call(
        functools.partial(kernel, n, length * n, batch, length, cuts, per, pitch),
        out_shape=[
            pltpu.VMEM((batch, length, head * LANES), bf16),
            pltpu.VMEM((late, SUBS * pitch, LANES), f32),
            pltpu.VMEM((late, SUBS * pitch, LANES), f32),
            pltpu.VMEM((late, LANES), f32),
        ],
        in_specs=[hbm] * 3,
        out_specs=[vmem] * 4,
        scratch_shapes=[
            pltpu.VMEM(leak_rate.shape, f32),
            pltpu.VMEM(leak_rate.shape, signal_in.dtype),
            pltpu.VMEM(leak_rate.shape, gate_in.dtype),
            spread, spread, spread, spread, spread, spread,
            pltpu.VMEM((units, 4, SUBS, LANES), f32),
            pltpu.VMEM((2 * units, LANES), f32),
            pltpu.VMEM((n, 2 * units, LANES), f32),
            pltpu.VMEM((2 * units, LANES), f32),
            pltpu.VMEM((n, 2 * units, LANES), f32),
            pltpu.VMEM((units, LANES), f32),
            pltpu.VMEM((units, LANES), f32),
        ],
        compiler_params=pltpu.CompilerParams(collective_id=0, has_side_effects=True),
    )(leak_rate, signal_in, gate_in)
    return pl.pallas_call(
        functools.partial(write, batch, length // SUBS, pitch),
        out_shape=jax.ShapeDtypeStruct(leak_rate.shape, bf16),
        in_specs=[vmem] * 4,
        out_specs=hbm,
        scratch_shapes=[pltpu.VMEM((batch, length, channels - head * LANES), bf16)],
        compiler_params=pltpu.CompilerParams(vmem_limit_bytes=4 << 20),
    )(*parts)


def solution(mesh):
    spec = P("copy", "span", "cols")
    return jax.shard_map(body, mesh=mesh, in_specs=(spec,) * 3, out_specs=spec, check_vma=False)
```

```python
import functools
import math

import jax
import jax.numpy as jnp
from jax import lax
from jax.experimental import pallas as pl
from jax.experimental.pallas import tpu as pltpu
from jax.sharding import PartitionSpec as P

LANES = 128
SUBS = 8
MESH = pl.DeviceIdType.MESH


def kernel(
    n, total, batch, length, cuts, per, pitch,
    leak_hbm, signal_hbm, gate_hbm, out_ref, base_ref, slope_ref, state_ref,
    leak_v, signal_v, gate_v, keep_s, push_s, silu_s, w_s, u_s, v_s, local_s,
    left_s, left_r, right_s, right_r, ahead_s, behind_s,
):
    def whole(sems, recv, ready):
        steps = length // SUBS
        tiles = cuts[-1]
        units = tiles * batch
        head = cuts[1] * batch
        trips = tiles // per

        def fetch(which, i):
            source = (leak_hbm, signal_hbm)[which]
            target = (leak_v, signal_v)[which]
            lanes = pl.ds(cuts[i] * LANES, (cuts[i + 1] - cuts[i]) * LANES)
            return pltpu.make_async_copy(
                source.at[:, :, lanes], target.at[:, :, lanes], sems.at[i]
            )

        def loaded(i):
            both = leak_v.at[:, pl.ds(0, length * 3 // 4), pl.ds(0, 2 * (cuts[i + 1] - cuts[i]) * LANES)]
            pltpu.make_async_copy(both, both, sems.at[i]).wait()

        for i in range(len(cuts) - 1):
            fetch(0, i).start()
            fetch(1, i).start()

        me = lax.axis_index("span")
        first, edge = me == 0, me == n - 1

        def left(sems, source, p, start, size, second=False):
            return pltpu.make_async_remote_copy(
                src_ref=left_s.at[pl.ds(start, size)],
                dst_ref=left_r.at[source, pl.ds(start, size)],
                send_sem=sems.at[source if second else p],
                recv_sem=recv.at[p if second else source],
                device_id={"span": p},
                device_id_type=MESH,
            )

        def right(sems, source, p, size):
            return pltpu.make_async_remote_copy(
                src_ref=right_s.at[pl.ds(0, size)],
                dst_ref=right_r.at[source, pl.ds(0, size)],
                send_sem=sems.at[p],
                recv_sem=recv.at[source],
                device_id={"span": p},
                device_id_type=MESH,
            )

        zero = jnp.zeros((units, LANES), jnp.float32)

        def begin():
            def each(begin, end, act):
                lax.fori_loop(begin, end, lambda p, x: (act(p), x)[1], 0)

            barrier = pltpu.get_barrier_semaphore()

            def greet(p):
                pl.semaphore_signal(barrier, inc=1, device_id={"span": p}, device_id_type=MESH)

            def arrived(p):
                pl.semaphore_signal(ready, inc=1, device_id={"span": p}, device_id_type=MESH)

            each(me + 1, n, greet)

            @pl.when(~first)
            def _():
                pl.semaphore_wait(barrier, me)

            each(0, me, arrived)

            def spread(target, u, value):
                for s in range(SUBS):
                    target[u, pl.ds(s * pitch, steps), :] = value[s * steps:(s + 1) * steps]

            def at(ref, u, k):
                return ref[u, pl.ds(k, SUBS, stride=pitch), :]

            place = lax.broadcasted_iota(jnp.int32, (SUBS, LANES), 0)

            def from_before(x, d, fill):
                return jnp.where(place < d, fill, pltpu.roll(x, d, 0))

            def from_after(x, d, fill):
                return jnp.where(place >= SUBS - d, fill, pltpu.roll(x, SUBS - d, 0))

            rate = -math.log2(math.e) / total

            def sweep(u, pieces):
                b, lanes = u % batch, pl.ds(u // batch * LANES, LANES)
                spread(keep_s, u, jnp.exp2(leak_v[b, :, lanes] * rate))
                spread(push_s, u, signal_v[b, :, lanes].astype(jnp.float32))
                size = steps // pieces
                g, q = [], []
                for i in range(pieces):
                    g.append(at(push_s, u, i * size))
                    q.append(at(keep_s, u, i * size))
                for k in range(1, size):
                    for i in range(pieces):
                        g[i] = g[i] + q[i] * at(push_s, u, i * size + k)
                        q[i] = q[i] * at(keep_s, u, i * size + k)
                for i in range(1, pieces):
                    g[0], q[0] = g[0] + q[0] * g[i], q[0] * q[i]
                local_s[u, 1] = g[0]
                local_s[u, 2] = q[0]
                return u, g[0], q[0]

            def total_of(u, g, q):
                d = 1
                while d < SUBS:
                    g = g + q * pltpu.roll(g, SUBS - d, 0)
                    q = q * pltpu.roll(q, SUBS - d, 0)
                    d *= 2
                left_s[u:u + 1] = g[:1]

            swept = []
            for i in range(len(cuts) - 1):
                loaded(i)
                here = range(cuts[i] * batch, cuts[i + 1] * batch)
                final = here.stop == units
                now = [sweep(u, 2 if final else 1) for u in here]
                if final or here.stop == head:
                    swept, now = swept + now, []
                for one in swept:
                    total_of(*one)
                swept = now
                if here.stop == head:
                    @pl.when(edge)
                    def _():
                        left(sems, me, 0, 0, head).start()

            @pl.when(edge)
            def _():
                left(sems, me, 0, head, units - head, True).start()

            gates = pltpu.make_async_copy(gate_hbm, gate_v, sems.at[n])
            gates.start()

            def rightward(t, carry):
                for i in range(per * batch):
                    u = t * (per * batch) + i
                    f = at(push_s, u, 0)
                    for k in range(1, steps):
                        f = at(keep_s, u, k) * f + at(push_s, u, k)
                    g, q = local_s[u, 1], local_s[u, 2]
                    a = q
                    d = 1
                    while d < SUBS:
                        f = f + q * from_before(f, d, 0.0)
                        g = g + a * from_after(g, d, 0.0)
                        q = q * from_before(q, d, 1.0)
                        a = a * from_after(a, d, 1.0)
                        d *= 2
                    local_s[u, 0] = f
                    local_s[u, 1] = g
                    local_s[u, 2] = q
                    local_s[u, 3] = a
                    right_s[pl.ds(u, 1), :] = f[SUBS - 1:]
                    right_s[pl.ds(units + u, 1), :] = q[SUBS - 1:]
                    left_s[pl.ds(units + u, 1), :] = a[:1]
                return carry

            lax.fori_loop(0, trips, rightward, 0)

            @pl.when(edge)
            def _():
                each(1, me, lambda p: left(sems, me, p, 0, units).start())

            @pl.when(~edge)
            def _():
                each(0, me, lambda p: left(sems, me, p, 0, 2 * units).start())

            scale = total ** (-0.5)
            gates.wait()

            def second(t, carry):
                for i in range(per * batch):
                    u = t * (per * batch) + i
                    lanes = pl.ds(pl.multiple_of((t * per + i // batch) * LANES, LANES), LANES)
                    x = gate_v[i % batch, :, lanes].astype(jnp.float32)
                    spread(silu_s, u, (x * scale) / (1.0 + jnp.exp(-x)))
                for i in range(per * batch):
                    u = t * (per * batch) + i
                    f = from_before(local_s[u, 0], 1, 0.0)
                    a = from_before(local_s[u, 2], 1, 1.0)
                    for k in range(steps):
                        keep = at(keep_s, u, k)
                        f = keep * f + at(push_s, u, k)
                        a = a * keep
                        w_s[u, pl.ds(k, SUBS, stride=pitch), :] = f
                        u_s[u, pl.ds(k, SUBS, stride=pitch), :] = a * at(silu_s, u, k)
                    g = from_after(local_s[u, 1], 1, 0.0)
                    a = from_after(local_s[u, 3], 1, 1.0)
                    for k in reversed(range(steps)):
                        keep, silu = at(keep_s, u, k), at(silu_s, u, k)
                        g = keep * g + at(push_s, u, k)
                        a = a * keep
                        w_s[u, pl.ds(k, SUBS, stride=pitch), :] = (at(w_s, u, k) + g) * silu
                        v_s[u, pl.ds(k, SUBS, stride=pitch), :] = a * silu
                return carry

            lax.fori_loop(0, trips, second, 0)

            @pl.when(~edge)
            def _():
                pl.semaphore_wait(ready, n - 1 - me)

            @pl.when(first)
            def _():
                each(1, n, lambda p: right(sems, me, p, units).start())

            @pl.when(~first)
            def _():
                each(me + 1, n, lambda p: right(sems, me, p, 2 * units).start())

            @pl.when(~first)
            def _():
                def join(i, state):
                    s, q = state
                    j = me - i
                    right(sems, j, me, 2 * units).wait_recv()
                    return s + q * right_r[j, :units], q * right_r[j, units:]

                s, q = lax.fori_loop(1, me, join, (zero, zero + 1.0))
                right(sems, 0, me, units).wait_recv()
                ahead_s[...] = s + q * right_r[0, :units]

                def entering(t, carry):
                    for i in range(per * batch):
                        u = t * (per * batch) + i
                        ahead = ahead_s[pl.ds(u, 1), :]
                        for s in range(SUBS):
                            rows = pl.ds(s * pitch, steps)
                            w_s[u, rows, :] = w_s[u, rows, :] + u_s[u, rows, :] * ahead
                    return carry

                lax.fori_loop(0, trips, entering, 0)

            @pl.when(edge)
            def _():
                left(sems, me, 0, 0, head).wait_send()
                left(sems, me, 0, head, units - head, True).wait_send()
                each(1, me, lambda p: left(sems, me, p, 0, units).wait_send())

            @pl.when(~edge)
            def _():
                each(0, me, lambda p: left(sems, me, p, 0, 2 * units).wait_send())

            @pl.when(first)
            def _():
                each(1, n, lambda p: right(sems, me, p, units).wait_send())

            @pl.when(~first)
            def _():
                each(me + 1, n, lambda p: right(sems, me, p, 2 * units).wait_send())

        begin()

        for u in range(head, units):
            base_ref[u - head] = w_s[u]
            slope_ref[u - head] = v_s[u]

        def join(j, state):
            s, q = state
            left(recv, j, me, 0, 2 * units).wait_recv()
            return s + q * left_r[j, :units], q * left_r[j, units:]

        near, far = lax.fori_loop(me + 1, n - 1, join, (zero, zero + 1.0))

        def behind(ref, begin, end):
            ref[0:end - begin] = (
                near[begin:end] + far[begin:end] * left_r[n - 1, begin:end]
            )

        @pl.when(edge)
        def _():
            behind_s[...] = zero
            state_ref[...] = zero[head:]

        @pl.when(~first & ~edge)
        def _():
            left(recv, n - 1, me, 0, units).wait_recv()
            behind(behind_s, 0, head)
            behind(state_ref, head, units)

        @pl.when(first)
        def _():
            left(recv, n - 1, 0, 0, head).wait_recv()
            behind(behind_s, 0, head)

        for u in range(head):
            b, lanes = u % batch, pl.ds(u // batch * LANES, LANES)
            state = behind_s[u:u + 1]
            for s in range(SUBS):
                rows = pl.ds(s * pitch, steps)
                out_ref[b, pl.ds(s * steps, steps), lanes] = (
                    w_s[u, rows, :] + v_s[u, rows, :] * state
                ).astype(out_ref.dtype)

        @pl.when(first)
        def _():
            left(recv, n - 1, 0, head, units - head, True).wait_recv()
            behind(state_ref, head, units)

    pl.run_scoped(
        whole,
        pltpu.SemaphoreType.DMA((max(len(cuts) - 1, n + 1),)),
        pltpu.SemaphoreType.DMA((n,)),
        pltpu.SemaphoreType.REGULAR,
    )


def write(
    batch, steps, pitch, done_ref, base_ref, slope_ref, state_ref, out_hbm, tail_v
):
    done, channels = done_ref.shape[2], out_hbm.shape[2]

    def put(sem):
        early = pltpu.make_async_copy(done_ref, out_hbm.at[:, :, pl.ds(0, done)], sem.at[0])
        late = pltpu.make_async_copy(
            tail_v, out_hbm.at[:, :, pl.ds(done, channels - done)], sem.at[1]
        )
        early.start()
        for u in range(base_ref.shape[0]):
            b, lanes = u % batch, pl.ds(u // batch * LANES, LANES)
            state = state_ref[u:u + 1]
            for s in range(SUBS):
                rows = pl.ds(s * pitch, steps)
                tail_v[b, pl.ds(s * steps, steps), lanes] = (
                    base_ref[u, rows, :] + slope_ref[u, rows, :] * state
                ).astype(tail_v.dtype)
        late.start()
        early.wait()
        late.wait()

    pl.run_scoped(put, pltpu.SemaphoreType.DMA((2,)))


def body(leak_rate, signal_in, gate_in):
    n = lax.axis_size("span")
    batch, length, channels = leak_rate.shape
    tiles = channels // LANES
    cuts = sorted({0, *(-(-tiles * share // 10) for share in (4, 7, 9, 10))})
    per = 2 if tiles % 2 == 0 else 1
    units = tiles * batch
    pitch = length // SUBS + 4
    hbm = pl.BlockSpec(memory_space=pl.ANY)
    f32 = jnp.float32
    spread = pltpu.VMEM((units, SUBS * pitch, LANES), f32)
    head = cuts[1]
    late = (tiles - head) * batch
    vmem = pl.BlockSpec(memory_space=pltpu.VMEM)
    bf16 = jnp.bfloat16
    parts = pl.pallas_call(
        functools.partial(kernel, n, length * n, batch, length, cuts, per, pitch),
        out_shape=[
            pltpu.VMEM((batch, length, head * LANES), bf16),
            pltpu.VMEM((late, SUBS * pitch, LANES), f32),
            pltpu.VMEM((late, SUBS * pitch, LANES), f32),
            pltpu.VMEM((late, LANES), f32),
        ],
        in_specs=[hbm] * 3,
        out_specs=[vmem] * 4,
        scratch_shapes=[
            pltpu.VMEM(leak_rate.shape, f32),
            pltpu.VMEM(leak_rate.shape, signal_in.dtype),
            pltpu.VMEM(leak_rate.shape, gate_in.dtype),
            spread, spread, spread, spread, spread, spread,
            pltpu.VMEM((units, 4, SUBS, LANES), f32),
            pltpu.VMEM((2 * units, LANES), f32),
            pltpu.VMEM((n, 2 * units, LANES), f32),
            pltpu.VMEM((2 * units, LANES), f32),
            pltpu.VMEM((n, 2 * units, LANES), f32),
            pltpu.VMEM((units, LANES), f32),
            pltpu.VMEM((units, LANES), f32),
        ],
        compiler_params=pltpu.CompilerParams(collective_id=0, has_side_effects=True),
    )(leak_rate, signal_in, gate_in)
    return pl.pallas_call(
        functools.partial(write, batch, length // SUBS, pitch),
        out_shape=jax.ShapeDtypeStruct(leak_rate.shape, bf16),
        in_specs=[vmem] * 4,
        out_specs=hbm,
        scratch_shapes=[pltpu.VMEM((batch, length, channels - head * LANES), bf16)],
        compiler_params=pltpu.CompilerParams(vmem_limit_bytes=4 << 20),
    )(*parts)


def solution(mesh):
    spec = P("copy", "span", "cols")
    return jax.shard_map(body, mesh=mesh, in_specs=(spec,) * 3, out_specs=spec, check_vma=False)
```
